32 devices in a mesh: band: 4 (over y, x), blk: 8 (over z, core).
Axes of the slice: x: 2, y: 2, z: 4, core: 2. Of those that a mesh axis runs over, the one named last changes fastest.
Arguments:
- solution: float32 [9, 2, 256, 2048], P(None, None, 'blk', 'band'), may hold values from -6 to 6
- residual: float32 [9, 2, 256, 2048], P(None, None, 'blk', 'band'), may hold values from -20 to 20
- direction: float32 [9, 2, 256, 2048], P(None, None, 'blk', 'band'), may hold values from -20 to 20
- precond: float32 [9, 2048], P(None, 'band'), may hold values from 0.2 to 2
- inv_spec: float32 [9, 2048], P(None, 'band'), may hold values from 0.05 to 2
- mixing: float32 [9, 3], replicated, may hold values from 0.1 to 2.5
- beams: float32 [9, 2048], replicated, may hold values from 0.2 to 1
- slot_band: int32 [12], replicated, may hold values from 0 to 11, each once
- m_order: int32 [256], replicated, may hold values from 0 to 255, each once
- cycle_order: int32 [128], replicated, may hold values from 0 to 127, each once
- inv_noise: float32 [12, 3, 128, 512], P('band', None, 'blk'), may hold values from 0.3 to 3
- pix_mask: int32 [128, 512], P('blk'), may hold values 0 or 1
Outputs:
- solution_next: float32 [9, 2, 256, 2048], P(None, None, 'blk', 'band')
- residual_next: float32 [9, 2, 256, 2048], P(None, None, 'blk', 'band')
- direction_next: float32 [9, 2, 256, 2048], P(None, None, 'blk', 'band')
The draws below stay inside these ranges and needn't reach their ends.
Inputs may be any that keep to these rules, and one draw needn't show every extreme that they name: `slot_band`: slots holding a value of 9 or more are empty; each band lies in exactly one slot. `m_order`: each order 0 to 255 appears once. `cycle_order`: each cycle 0 to 127 appears once.
All inputs are finite; a program needn't handle non-finite values. No bound on the sum of `pix_mask` on one device may be relied on, other than what follows from the above.
Results may differ from the reference program's by a relative error of at most 0.0075.
Values may be sent and summed in bfloat16 or wider, within the bound.
A program may use at most 128 MiB of HBM per device.

```python
import math
import jax
import jax.numpy as jnp
from jax import lax

COMP = 3
STOKES = 3
FIELDS = 9
BANDS = 9
SLOTS_ALL = 12
L = 2048
M_DEV = 32
MODES = 256
CYCLES = 128
PHI = 512


def rising_field(key, salt):
    folded = jax.random.fold_in(key, salt)
    base = jax.random.truncated_normal(folded, -4.0, 4.0, (FIELDS, 2, MODES, L), jnp.float32)
    m_rise = 0.5 + jnp.arange(MODES, dtype=jnp.float32) / MODES
    l_rise = 0.5 + jnp.arange(L, dtype=jnp.float32) / L
    block_total = MODES // M_DEV
    block_key = jax.random.fold_in(folded, 3)
    block_scale = jnp.exp(jax.random.uniform(block_key, (block_total,), jnp.float32, math.log(0.4), math.log(2.5)))
    scaling = m_rise[:, None] * l_rise[None, :]
    row_scale = jnp.repeat(block_scale, M_DEV)
    scaling = scaling * row_scale[:, None]
    return jnp.clip(base * scaling, -20.0, 20.0)


def draw_residual(key, part):
    return rising_field(key, 11)


def draw_direction(key, part):
    return rising_field(key, 23)


def touch_ends(entries, key, least, high):
    place = [jax.random.randint(jax.random.fold_in(key, axis), (), 0, length) for axis, length in enumerate(entries.shape)]
    main_axis = entries.shape.index(max(entries.shape))
    next_to = place[:main_axis] + [(place[main_axis] + 1) % entries.shape[main_axis]] + place[main_axis + 1:]
    return entries.at[tuple(place)].set(least).at[tuple(next_to)].set(high)


def block_levels(stream_key, shape, cuts, low, largest):
    def one(axis_at, parts):
        steps = jax.random.uniform(jax.random.fold_in(jax.random.fold_in(stream_key, 6), axis_at), (parts,), jnp.float32, low / len(cuts), largest / len(cuts))
        return jnp.repeat(jnp.exp(steps), shape[axis_at] // parts).reshape((-1,) + (1,) * (len(shape) - axis_at - 1))

    level = one(*cuts[0])
    for cut in cuts[1:]:
        level = level * one(*cut)
    return level


def gaussian(own_key, shape, deviation, limit, split=(), held_as=jnp.bfloat16):
    gain = block_levels(own_key, shape, split, -0.22, 0.18) if split else 1.0
    drawn = jax.random.normal(own_key, shape, jnp.float32) * deviation * gain
    return jnp.minimum(jnp.maximum(drawn, -limit), limit).astype(held_as)


def setup_inputs(seed: int = 0) -> dict:
    key_list = jax.random.split(jax.random.key(seed), 13)
    return {
        "solution": gaussian(key_list[0], (FIELDS, 2, MODES, L), 1.0, 6.0, ((2, 8), (3, 4)), jnp.float32),
        "residual": draw_residual(jax.random.fold_in(key_list[12], 71), 0),
        "direction": draw_direction(jax.random.fold_in(key_list[12], 71), 0),
        "precond": jnp.clip(jnp.exp(math.log(2.0) - 2.3025851 * jax.random.uniform(key_list[3], (FIELDS, L), jnp.float32) ** block_levels(key_list[3], (FIELDS, L), ((1, 4),), -0.2, 0.2)), 0.2, 2.0),
        "inv_spec": jnp.clip(jnp.exp(math.log(2.0) - 3.6888794 * jax.random.uniform(key_list[4], (FIELDS, L), jnp.float32) ** block_levels(key_list[4], (FIELDS, L), ((1, 4),), -0.2, 0.2)), 0.05, 2.0),
        "mixing": jnp.clip(jnp.exp(jax.random.uniform(key_list[5], (BANDS, COMP), jnp.float32, math.log(0.1), math.log(2.5))), 0.1, 2.5),
        "beams": jnp.clip(jnp.exp(jax.random.uniform(key_list[6], (BANDS, L), jnp.float32, math.log(0.2), math.log(1.0))), 0.2, 1.0),
        "slot_band": jax.random.permutation(key_list[7], SLOTS_ALL).astype(jnp.int32),
        "m_order": jax.random.permutation(key_list[8], MODES).astype(jnp.int32),
        "cycle_order": jax.random.permutation(key_list[9], CYCLES).astype(jnp.int32),
        "inv_noise": jnp.clip(jnp.exp(math.log(3.0) - 2.3025851 * jax.random.uniform(key_list[10], (SLOTS_ALL, STOKES, CYCLES, PHI), jnp.float32) ** block_levels(key_list[10], (SLOTS_ALL, STOKES, CYCLES, PHI), ((0, 4), (2, 8)), -0.2, 0.2)), 0.3, 3.0),
        "pix_mask": touch_ends((jax.random.randint(key_list[11], (CYCLES, PHI), 0, 4) < 3).astype(jnp.int32), jax.random.fold_in(key_list[11], 1), 0, 1),
    }


def rounded(values):
    return lax.optimization_barrier(values.astype(jnp.bfloat16)).astype(jnp.float32)

def legendre_table(cycle_order, l_total, cycle_total):
    l_values = jnp.arange(l_total, dtype=jnp.int32)
    phase_int = l_values[None, :] * (2 * cycle_order[:, None] + 1) % (4 * cycle_total)
    angles = phase_int.astype(jnp.float32) * (math.pi / (2 * cycle_total))
    return (jnp.cos(angles) / math.sqrt(l_total)).astype(jnp.bfloat16)

def fourier_block(m_order, first_cell, block_width, phi_total):
    phi_cells = first_cell + jnp.arange(block_width, dtype=jnp.int32)
    phase_int = m_order[:, None] * phi_cells[None, :] % phi_total
    angles = phase_int.astype(jnp.float32) * (2.0 * math.pi / phi_total)
    scaling = 1.0 / math.sqrt(m_order.shape[0])
    return jnp.stack([jnp.cos(angles) * scaling, -jnp.sin(angles) * scaling]).astype(jnp.bfloat16)

def reference(solution, residual, direction, precond, inv_spec, mixing, beams, slot_band, m_order, cycle_order, inv_noise, pix_mask):
    highest = lax.Precision.HIGHEST
    colat = legendre_table(cycle_order, L, CYCLES).astype(jnp.float32)
    azim = fourier_block(m_order, 0, PHI, PHI).astype(jnp.float32)
    triangle = (jnp.arange(L, dtype=jnp.int32)[None, :] >= m_order[:, None]).astype(jnp.float32)
    select = (slot_band[:, None] == jnp.arange(BANDS, dtype=jnp.int32)[None, :]).astype(jnp.float32)
    slot_mix = jnp.dot(select, mixing, precision=highest)
    slot_beam = jnp.dot(select, beams, precision=highest)
    halved = direction.astype(jnp.bfloat16).astype(jnp.float32).reshape(COMP, STOKES, 2, MODES, L)
    weight = inv_noise * pix_mask.astype(jnp.float32)[None, None]

    def one_slot(running, slot_index):
        mix_row = slot_mix[slot_index]
        beam_row = slot_beam[slot_index]
        mixed_sum = lax.optimization_barrier(jnp.sum(mix_row[:, None, None, None, None] * halved, axis=0))
        amplitudes = rounded(mixed_sum * beam_row[None, None, None, :] * triangle[None, None])
        colat_side = rounded(jnp.einsum('xkml,rl->xkmr', amplitudes, colat, precision=highest))
        sky_part = jnp.einsum('xkmr,kmp->xrp', colat_side, azim, precision=highest)
        weighted = rounded(weight[slot_index] * sky_part)
        back_cycle = rounded(jnp.einsum('xrp,kmp->xkmr', weighted, azim, precision=highest))
        back_harm = jnp.einsum('xkmr,rl->xkml', back_cycle, colat, precision=highest)
        back_harm = back_harm * beam_row[None, None, None, :] * triangle[None, None]
        term = mix_row[:, None, None, None, None] * back_harm[None]
        return (running + term.reshape(FIELDS, 2, MODES, L), None)
    zero_carry = jnp.zeros((FIELDS, 2, MODES, L), jnp.float32)
    band_term, _ = lax.scan(one_slot, zero_carry, jnp.arange(SLOTS_ALL, dtype=jnp.int32))
    prior_diag = inv_spec[:, None, None, :]
    precond_full = precond[:, None, None, :]
    applied = prior_diag * direction + band_term
    scaled_res = precond_full * residual
    norm_old = jnp.sum(residual * scaled_res)
    curvature = jnp.sum(direction * applied)
    step_size = norm_old / curvature
    solution_next = solution + step_size * direction
    residual_next = residual - step_size * applied
    scaled_next = precond_full * residual_next
    norm_new = jnp.sum(residual_next * scaled_next)
    direction_next = scaled_next + norm_new / norm_old * direction
    return (solution_next, residual_next, direction_next)
```

```python
import functools
import math

import jax
import jax.numpy as jnp
from jax import lax
from jax.experimental import pallas as pl
from jax.experimental.pallas import tpu as pltpu
from jax.sharding import PartitionSpec as P

COMP = 3
STOKES = 3
FIELDS = 9
BANDS = 9
LANES = 512
MESH = pl.DeviceIdType.MESH


def wave(phase, quarter):
    folded = jnp.abs(phase - 2 * quarter) - quarter
    x = folded.astype(jnp.float32) * (math.pi / (2 * quarter))
    x2 = x * x
    series = -1.0 / 39916800.0
    for coefficient in (1.0 / 362880.0, -1.0 / 5040.0, 1.0 / 120.0, -1.0 / 6.0, 1.0):
        series = series * x2 + coefficient
    return x * series


def wrapped(value, period):
    if period & (period - 1) == 0:
        return value & (period - 1)
    return lax.rem(value, period)


def contract(left, right, left_dim, right_dim):
    return lax.dot_general(
        left, right, (((left_dim,), (right_dim,)), ((), ())), preferred_element_type=jnp.float32
    )


def wait_bytes(ref, sem):
    pltpu.make_async_copy(ref, ref, sem).wait()


def kernel(
    sizes,
    direction,
    residual,
    precond,
    inv_spec,
    slot_mix,
    slot_beam,
    my_orders,
    all_orders,
    cycles,
    noise,
    mask,
    applied,
    totals,
    tri,
    halved,
    colat,
    amps,
    send,
    recv,
    azim,
    side,
    back,
    back_send,
    back_recv,
    stats,
    send_sem,
    recv_sem,
    back_send_sem,
    back_recv_sem,
    stat_send_sem,
    stat_recv_sem,
):
    groups, blocks, slots, l_total, modes, phi_total = sizes
    rows, l_local = direction.shape[1:]
    cycle_total = cycles.shape[0]
    r_local = cycle_total // blocks
    pairs = slots * STOKES
    per_lane = 128 // rows
    my_band = lax.axis_index("band")
    my_block = lax.axis_index("blk")

    def target(step, shift):
        return (lax.rem(my_band + step, groups), lax.rem(my_block + shift, blocks))

    barrier = pltpu.get_barrier_semaphore()

    def greet(flat, carry):
        pl.semaphore_signal(
            barrier, inc=1, device_id=target(flat // blocks, flat % blocks), device_id_type=MESH
        )
        return carry

    lax.fori_loop(1, groups * blocks, greet, 0)

    l_index = my_band * l_local + lax.broadcasted_iota(jnp.int32, (1, l_local), 1)
    tri[...] = jnp.where(l_index >= my_orders[...], 1.0, 0.0)
    for field in range(FIELDS):
        halved[field] = direction[field].astype(jnp.bfloat16).astype(jnp.float32) * tri[...]

    def colat_rows(at, carry):
        at_rows = pl.ds(pl.multiple_of(at * 64, 64), 64)
        phase = wrapped(l_index * (2 * cycles[at_rows, :] + 1), 4 * cycle_total)
        colat[at_rows, :] = (wave(phase, cycle_total) / math.sqrt(l_total)).astype(jnp.bfloat16)
        return carry

    lax.fori_loop(0, cycle_total // 64, colat_rows, 0)

    def transform(step):
        group = lax.rem(my_band + step, groups)
        for slot in range(slots):
            at = group * slots + slot
            beam = slot_beam[at]
            for stokes in range(STOKES):
                mixed = slot_mix[at * COMP] * halved[stokes]
                for comp in range(1, COMP):
                    mixed = mixed + slot_mix[at * COMP + comp] * halved[comp * STOKES + stokes]
                first = (slot * STOKES + stokes) * rows
                amps[first : first + rows, :] = (mixed * beam).astype(jnp.bfloat16)
        send[step] = contract(colat[...], amps[...], 1, 1).astype(jnp.bfloat16)

    def block_rows(block):
        return pl.ds(pl.multiple_of(block * r_local, r_local), r_local)

    def ship(step, shift):
        there = target(step, shift)
        pltpu.make_async_remote_copy(
            src_ref=send.at[step, block_rows(there[1])],
            dst_ref=recv.at[step, block_rows(shift)],
            send_sem=send_sem.at[step],
            recv_sem=recv_sem.at[step],
            device_id=there,
            device_id_type=MESH,
        ).start()

    def ship_from(step, first):
        def one(shift, carry):
            ship(step, shift)
            return carry

        lax.fori_loop(first, blocks, one, 0)

    transform(1)
    pl.semaphore_wait(barrier, groups * blocks - 1)
    ship_from(1, 0)

    def group_step(step, carry):
        transform(step)
        ship_from(step, 0)
        return carry

    lax.fori_loop(2, groups, group_step, 0)
    transform(0)
    ship_from(0, 1)
    recv[0, 0:r_local] = send[0, block_rows(my_block)]

    def fill_azim(chunk):
        cell = chunk * LANES + lax.broadcasted_iota(jnp.int32, (1, LANES), 1)

        def one(at, carry):
            at_rows = pl.ds(pl.multiple_of(at * 2 * rows, 2 * rows), 2 * rows)
            turned = lax.broadcasted_iota(jnp.int32, (2 * rows, 1), 0) % rows >= rows // 2
            shift = jnp.where(turned, phi_total // 4, 0)
            phase = wrapped(all_orders[at_rows, :] * cell + shift, phi_total)
            azim[at_rows, :] = (wave(phase, phi_total // 4) / math.sqrt(modes)).astype(jnp.bfloat16)
            return carry

        lax.fori_loop(0, blocks // 2, one, 0)

    chunks = phi_total // LANES
    if chunks == 1:
        fill_azim(0)
    residual_sum = jnp.zeros((rows, l_local), jnp.float32)
    for field in range(FIELDS):
        residual_sum = residual_sum + residual[field] * (precond[field] * residual[field])

    rest = (blocks - 1) * r_local
    wait_bytes(recv.at[0, 0:rest], recv_sem.at[0])
    wait_bytes(recv.at[1], recv_sem.at[1])
    for step in range(2, groups):
        wait_bytes(recv.at[step], recv_sem.at[step])

    def gather(at, carry):
        parts = []
        for inner in range(per_lane):
            block = at * per_lane + inner
            rows_at = block_rows(lax.rem(my_block - block + blocks, blocks))
            total = recv[0, rows_at, :].astype(jnp.float32)
            for step in range(1, groups):
                total = total + recv[step, rows_at, :].astype(jnp.float32)
            parts.append(total)
        columns = pl.ds(pl.multiple_of(at * 128, 128), 128)
        for pair in range(pairs):
            picked = [part[:, pair * rows : (pair + 1) * rows] for part in parts]
            joined = jnp.concatenate(picked, axis=1).astype(jnp.bfloat16)
            side[pair * r_local : (pair + 1) * r_local, columns] = joined
        return carry

    lax.fori_loop(0, blocks // per_lane, gather, 0)

    def weigh(chunk):
        columns = pl.ds(pl.multiple_of(chunk * LANES, LANES), LANES)
        sky = contract(side[...], azim[...], 1, 0).reshape(pairs, r_local, LANES)
        weight = noise[:, :, columns] * mask[:, columns].astype(jnp.float32)[None]
        weighted = (weight * sky).astype(jnp.bfloat16).reshape(pairs * r_local, LANES)
        return contract(weighted, azim[...], 1, 1)

    if chunks == 1:
        back[...] = weigh(0)
    else:
        back[...] = jnp.zeros_like(back)

        def one_chunk(chunk, carry):
            fill_azim(chunk)
            back[...] += weigh(chunk)
            return carry

        lax.fori_loop(0, chunks, one_chunk, 0)

    def scatter(at, carry):
        columns = pl.ds(pl.multiple_of(at * 128, 128), 128)
        wide = [back[pair * r_local : (pair + 1) * r_local, columns] for pair in range(pairs)]
        for inner in range(per_lane):
            picked = [part[:, inner * rows : (inner + 1) * rows] for part in wide]
            joined = jnp.concatenate(picked, axis=1).astype(jnp.bfloat16)
            back_send[at * per_lane + inner] = joined
        return carry

    lax.fori_loop(0, blocks // per_lane, scatter, 0)

    def return_to(step, shift):
        there = target(step, shift)
        pltpu.make_async_remote_copy(
            src_ref=back_send.at[there[1]],
            dst_ref=back_recv.at[step, block_rows(my_block)],
            send_sem=back_send_sem.at[step],
            recv_sem=back_recv_sem.at[step],
            device_id=there,
            device_id_type=MESH,
        ).start()

    def return_step(step, first):
        def one(shift, carry):
            return_to(step, shift)
            return carry

        lax.fori_loop(first, blocks, one, 0)

    return_step(0, 1)
    for step in range(1, groups):
        return_step(step, 0)
    back_recv[0, block_rows(my_block)] = back_send[my_block]
    applied[...] = jnp.zeros_like(applied)

    def combine(step):
        group = lax.rem(my_band - step + groups, groups)
        harm = contract(back_recv[step], colat[...], 0, 0)
        for stokes in range(STOKES):
            sums = [applied[comp * STOKES + stokes] for comp in range(COMP)]
            for slot in range(slots):
                at = group * slots + slot
                first = (slot * STOKES + stokes) * rows
                term = harm[first : first + rows, :] * slot_beam[at]
                sums = [sums[comp] + slot_mix[at * COMP + comp] * term for comp in range(COMP)]
            for comp in range(COMP):
                applied[comp * STOKES + stokes] = sums[comp]

    wait_bytes(back_recv.at[0, 0:rest], back_recv_sem.at[0])
    combine(0)

    def combine_step(step, carry):
        wait_bytes(back_recv.at[step], back_recv_sem.at[step])
        combine(step)
        return carry

    lax.fori_loop(1, groups, combine_step, 0)

    curvature = jnp.zeros((rows, l_local), jnp.float32)
    crossed = jnp.zeros((rows, l_local), jnp.float32)
    squared = jnp.zeros((rows, l_local), jnp.float32)
    for field in range(FIELDS):
        held = direction[field]
        value = inv_spec[field] * held + applied[field] * tri[...]
        applied[field] = value
        scaled = precond[field] * value
        curvature = curvature + held * value
        crossed = crossed + residual[field] * scaled
        squared = squared + value * scaled

    def lane_sums(value):
        row = jnp.sum(value, axis=0, keepdims=True)
        return functools.reduce(
            jnp.add, [row[:, at : at + 128] for at in range(0, l_local, 128)]
        )

    stats[0] = jnp.concatenate(
        [lane_sums(v) for v in (residual_sum, curvature, crossed, squared)]
        + [jnp.zeros((4, 128), jnp.float32)],
        axis=0,
    )

    def tell(flat, carry):
        pltpu.make_async_remote_copy(
            src_ref=stats.at[0],
            dst_ref=stats.at[flat],
            send_sem=stat_send_sem,
            recv_sem=stat_recv_sem,
            device_id=target(flat // blocks, flat % blocks),
            device_id_type=MESH,
        ).start()
        return carry

    lax.fori_loop(1, groups * blocks, tell, 0)
    wait_bytes(stats.at[1 : groups * blocks], stat_recv_sem)
    summed = jnp.sum(jnp.sum(stats[...], axis=0), axis=1, keepdims=True)
    totals[...] = jnp.broadcast_to(summed, totals.shape)

    wait_bytes(stats.at[1 : groups * blocks], stat_send_sem)
    wait_bytes(recv.at[0, 0:rest], send_sem.at[0])
    wait_bytes(back_recv.at[0, 0:rest], back_send_sem.at[0])
    for step in range(1, groups):
        wait_bytes(recv.at[step], send_sem.at[step])
        wait_bytes(back_recv.at[step], back_send_sem.at[step])


def on_device(
    solution,
    residual,
    direction,
    precond,
    inv_spec,
    mixing,
    beams,
    slot_band,
    m_order,
    cycle_order,
    inv_noise,
    pix_mask,
):
    band_index = lax.axis_index("band")
    block_index = lax.axis_index("blk")
    groups = lax.axis_size("band")
    blocks = lax.axis_size("blk")
    m_local, l_local = direction.shape[2:]
    rows = 2 * m_local
    modes = m_order.shape[0]
    cycle_total = cycle_order.shape[0]
    slots, _, r_local, phi_total = inv_noise.shape
    pairs = slots * STOKES
    devices = groups * blocks

    select = (slot_band[:, None] == jnp.arange(BANDS, dtype=jnp.int32)[None, :]).astype(jnp.float32)
    slot_mix = jnp.sum(select[:, :, None] * mixing[None], axis=1).reshape(-1)
    my_beams = lax.dynamic_slice_in_dim(beams, band_index * l_local, l_local, 1)
    slot_beam = jnp.sum(select[:, :, None] * my_beams[None], axis=1)[:, None, :]
    by_block = m_order.reshape(blocks, m_local)
    all_orders = jnp.concatenate([by_block, by_block], axis=1)
    my_orders = lax.dynamic_slice_in_dim(all_orders, block_index, 1).reshape(rows, 1)

    vmem = pl.BlockSpec(memory_space=pltpu.VMEM)
    smem = pl.BlockSpec(memory_space=pltpu.SMEM)
    bf16, f32 = jnp.bfloat16, jnp.float32
    field_shape = (FIELDS, rows, l_local)
    dma = pltpu.SemaphoreType.DMA
    sizes = (groups, blocks, slots, l_local * groups, modes, phi_total)
    applied, totals = pl.pallas_call(
        functools.partial(kernel, sizes),
        out_shape=(
            jax.ShapeDtypeStruct(field_shape, f32),
            jax.ShapeDtypeStruct((8, 128), f32),
        ),
        in_specs=[vmem] * 4 + [smem] + [vmem] * 6,
        out_specs=(vmem, vmem),
        scratch_shapes=[
            pltpu.VMEM((rows, l_local), f32),
            pltpu.VMEM(field_shape, f32),
            pltpu.VMEM((cycle_total, l_local), bf16),
            pltpu.VMEM((pairs * rows, l_local), bf16),
            pltpu.VMEM((groups, cycle_total, pairs * rows), bf16),
            pltpu.VMEM((groups, cycle_total, pairs * rows), bf16),
            pltpu.VMEM((blocks * rows, LANES), bf16),
            pltpu.VMEM((pairs * r_local, blocks * rows), bf16),
            pltpu.VMEM((pairs * r_local, blocks * rows), f32),
            pltpu.VMEM((blocks, r_local, pairs * rows), bf16),
            pltpu.VMEM((groups, cycle_total, pairs * rows), bf16),
            pltpu.VMEM((devices, 8, 128), f32),
            dma((groups,)),
            dma((groups,)),
            dma((groups,)),
            dma((groups,)),
            dma,
            dma,
        ],
        compiler_params=pltpu.CompilerParams(
            collective_id=0, has_side_effects=True, vmem_limit_bytes=60 * 1024 * 1024
        ),
    )(
        direction.reshape(field_shape),
        residual.reshape(field_shape),
        precond[:, None, :],
        inv_spec[:, None, :],
        slot_mix,
        slot_beam,
        my_orders,
        all_orders.reshape(blocks * rows, 1),
        cycle_order[:, None],
        inv_noise.reshape(pairs, r_local, phi_total),
        pix_mask,
    )
    applied = applied.reshape(direction.shape)
    norm_old, curvature, crossed, squared = (totals[at, 0] for at in range(4))
    precond_full = precond[:, None, None, :]
    step_size = norm_old / curvature
    solution_next = solution + step_size * direction
    residual_next = residual - step_size * applied
    norm_new = norm_old - 2.0 * step_size * crossed + step_size * step_size * squared
    direction_next = precond_full * residual_next + norm_new / norm_old * direction
    return (solution_next, residual_next, direction_next)


def solution(mesh):
    field = P(None, None, "blk", "band")
    return jax.shard_map(
        on_device,
        mesh=mesh,
        in_specs=(
            field,
            field,
            field,
            P(None, "band"),
            P(None, "band"),
            P(),
            P(),
            P(),
            P(),
            P(),
            P("band", None, "blk", None),
            P("blk", None),
        ),
        out_specs=(field, field, field),
        check_vma=False,
    )
```

```python
import functools
import math

import jax
import jax.numpy as jnp
from jax import lax
from jax.experimental import pallas as pl
from jax.experimental.pallas import tpu as pltpu
from jax.sharding import PartitionSpec as P

COMP = 3
STOKES = 3
FIELDS = 9
BANDS = 9
LANES = 512
MESH = pl.DeviceIdType.MESH


def wave(phase, quarter):
    folded = jnp.abs(phase - 2 * quarter) - quarter
    x = folded.astype(jnp.float32) * (math.pi / (2 * quarter))
    x2 = x * x
    series = -1.0 / 39916800.0
    for coefficient in (1.0 / 362880.0, -1.0 / 5040.0, 1.0 / 120.0, -1.0 / 6.0, 1.0):
        series = series * x2 + coefficient
    return x * series


def wrapped(value, period):
    if period & (period - 1) == 0:
        return value & (period - 1)
    return lax.rem(value, period)


def contract(left, right, left_dim, right_dim):
    return lax.dot_general(
        left, right, (((left_dim,), (right_dim,)), ((), ())), preferred_element_type=jnp.float32
    )


def wait_bytes(ref, sem):
    pltpu.make_async_copy(ref, ref, sem).wait()


def kernel(
    sizes,
    direction,
    residual,
    precond,
    inv_spec,
    mixing,
    slot_band,
    m_order,
    cycle_order,
    beams,
    noise,
    mask,
    applied,
    step_row,
    ratio_row,
    tri,
    halved,
    colat,
    amps,
    send,
    recv,
    joint,
    turned,
    azim,
    side,
    back,
    back_send,
    back_recv,
    stats,
    send_sem,
    recv_sem,
    turn_send_sem,
    turn_recv_sem,
    back_send_sem,
    back_recv_sem,
    spread_send_sem,
    spread_recv_sem,
    stat_send_sem,
    stat_recv_sem,
):
    groups, blocks, slots, l_total, modes, phi_total = sizes
    rows, l_local = direction.shape[1:]
    cycle_total = cycle_order.shape[0]
    r_local = cycle_total // blocks
    pairs = slots * STOKES
    per_lane = 128 // rows
    my_band = lax.axis_index("band")
    my_block = lax.axis_index("blk")

    def target(step, shift):
        return (lax.rem(my_band + step, groups), lax.rem(my_block + shift, blocks))

    barrier = pltpu.get_barrier_semaphore()

    def greet(flat, carry):
        pl.semaphore_signal(
            barrier, inc=1, device_id=target(flat // blocks, flat % blocks), device_id_type=MESH
        )
        return carry

    lax.fori_loop(1, groups * blocks, greet, 0)

    def slot_row(at):
        band = slot_band[at]
        filled = jnp.where(band < BANDS, 1.0, 0.0)
        held = jnp.minimum(band, BANDS - 1)
        columns = pl.ds(pl.multiple_of(my_band * l_local, l_local), l_local)
        mix = [filled * mixing[comp, held] for comp in range(COMP)]
        return (mix, beams[pl.ds(held, 1), columns])

    def column(ref, first, count, width):
        place = lax.broadcasted_iota(jnp.int32, (8, 128), 0)
        pieces = []
        for at in range(0, count, 8):
            piece = jnp.full((8, 128), ref[first + at], jnp.int32)
            for inner in range(1, 8):
                piece = jnp.where(place == inner, ref[first + at + inner], piece)
            pieces.append(piece)
        tall = jnp.concatenate(pieces, axis=0)
        return jnp.concatenate([tall] * (width // 128), axis=1)

    l_index = my_band * l_local + lax.broadcasted_iota(jnp.int32, (1, l_local), 1)
    my_orders = column(m_order, my_block * (rows // 2), rows // 2, l_local)
    tri[...] = jnp.where(l_index >= jnp.concatenate([my_orders, my_orders], axis=0), 1.0, 0.0)
    for field in range(FIELDS):
        halved[field] = direction[field].astype(jnp.bfloat16).astype(jnp.float32) * tri[...]

    def colat_rows(at, carry):
        at_rows = pl.ds(pl.multiple_of(at * 64, 64), 64)
        phase = wrapped(l_index * (2 * column(cycle_order, at * 64, 64, l_local) + 1), 4 * cycle_total)
        colat[at_rows, :] = (wave(phase, cycle_total) / math.sqrt(l_total)).astype(jnp.bfloat16)
        return carry

    lax.fori_loop(0, cycle_total // 64, colat_rows, 0)

    def transform(step):
        group = lax.rem(my_band + step, groups)
        for slot in range(slots):
            at = group * slots + slot
            mix, beam = slot_row(at)
            for stokes in range(STOKES):
                mixed = mix[0] * halved[stokes]
                for comp in range(1, COMP):
                    mixed = mixed + mix[comp] * halved[comp * STOKES + stokes]
                first = (slot * STOKES + stokes) * rows
                amps[first : first + rows, :] = (mixed * beam).astype(jnp.bfloat16)
        send[step] = contract(colat[...], amps[...], 1, 1).astype(jnp.bfloat16)

    def block_rows(block):
        return pl.ds(pl.multiple_of(block * r_local, r_local), r_local)

    def ship(step):
        pltpu.make_async_remote_copy(
            src_ref=send.at[step],
            dst_ref=recv.at[step],
            send_sem=send_sem.at[step],
            recv_sem=recv_sem.at[step],
            device_id=target(step, 0),
            device_id_type=MESH,
        ).start()

    transform(1)
    pl.semaphore_wait(barrier, groups * blocks - 1)
    ship(1)

    def group_step(step, carry):
        transform(step)
        ship(step)
        return carry

    lax.fori_loop(2, groups, group_step, 0)
    transform(0)

    def fill_azim(chunk):
        cell = chunk * LANES + lax.broadcasted_iota(jnp.int32, (1, LANES), 1)

        def one(at, carry):
            at_rows = pl.ds(pl.multiple_of(at * 2 * rows, 2 * rows), 2 * rows)
            phases = []
            for inner in range(2):
                orders = column(m_order, (at * 2 + inner) * (rows // 2), rows // 2, LANES)
                phases += [orders * cell, orders * cell + phi_total // 4]
            phase = wrapped(jnp.concatenate(phases, axis=0), phi_total)
            azim[at_rows, :] = (wave(phase, phi_total // 4) / math.sqrt(modes)).astype(jnp.bfloat16)
            return carry

        lax.fori_loop(0, blocks // 2, one, 0)

    chunks = phi_total // LANES
    if chunks == 1:
        fill_azim(0)
    rest = (blocks - 1) * r_local
    for step in range(1, groups):
        wait_bytes(recv.at[step], recv_sem.at[step])

    def add_up(at, carry):
        at_rows = block_rows(at)
        total = send[0, at_rows, :].astype(jnp.float32)
        for step in range(1, groups):
            total = total + recv[step, at_rows, :].astype(jnp.float32)
        joint[at_rows, :] = total.astype(jnp.bfloat16)
        return carry

    lax.fori_loop(0, blocks, add_up, 0)

    def turn(shift, carry):
        there = target(0, shift)
        pltpu.make_async_remote_copy(
            src_ref=joint.at[block_rows(there[1])],
            dst_ref=turned.at[block_rows(shift)],
            send_sem=turn_send_sem,
            recv_sem=turn_recv_sem,
            device_id=there,
            device_id_type=MESH,
        ).start()
        return carry

    lax.fori_loop(1, blocks, turn, 0)
    turned[0:r_local] = joint[block_rows(my_block)]
    residual_sum = jnp.zeros((rows, l_local), jnp.float32)
    for field in range(FIELDS):
        residual_sum = residual_sum + residual[field] * (
            precond[field : field + 1] * residual[field]
        )
    wait_bytes(turned.at[r_local:cycle_total], turn_recv_sem)

    def gather(at, carry):
        parts = []
        for inner in range(per_lane):
            block = at * per_lane + inner
            rows_at = block_rows(lax.rem(my_block - block + blocks, blocks))
            parts.append(turned[rows_at, :].astype(jnp.float32))
        columns = pl.ds(pl.multiple_of(at * 128, 128), 128)
        for pair in range(pairs):
            picked = [part[:, pair * rows : (pair + 1) * rows] for part in parts]
            joined = jnp.concatenate(picked, axis=1).astype(jnp.bfloat16)
            side[pair * r_local : (pair + 1) * r_local, columns] = joined
        return carry

    lax.fori_loop(0, blocks // per_lane, gather, 0)

    def weigh(chunk):
        columns = pl.ds(pl.multiple_of(chunk * LANES, LANES), LANES)
        sky = contract(side[...], azim[...], 1, 0).reshape(pairs, r_local, LANES)
        weight = noise[:, :, columns] * mask[:, columns].astype(jnp.float32)[None]
        weighted = (weight * sky).astype(jnp.bfloat16).reshape(pairs * r_local, LANES)
        return contract(weighted, azim[...], 1, 1)

    if chunks == 1:
        back[...] = weigh(0)
    else:
        back[...] = jnp.zeros_like(back)

        def one_chunk(chunk, carry):
            fill_azim(chunk)
            back[...] += weigh(chunk)
            return carry

        lax.fori_loop(0, chunks, one_chunk, 0)

    def scatter(at, carry):
        columns = pl.ds(pl.multiple_of(at * 128, 128), 128)
        wide = [back[pair * r_local : (pair + 1) * r_local, columns] for pair in range(pairs)]
        for inner in range(per_lane):
            picked = [part[:, inner * rows : (inner + 1) * rows] for part in wide]
            joined = jnp.concatenate(picked, axis=1).astype(jnp.bfloat16)
            back_send[at * per_lane + inner] = joined
        return carry

    lax.fori_loop(0, blocks // per_lane, scatter, 0)

    def return_to(shift, carry):
        there = target(0, shift)
        pltpu.make_async_remote_copy(
            src_ref=back_send.at[there[1]],
            dst_ref=back_recv.at[0, block_rows(my_block)],
            send_sem=back_send_sem,
            recv_sem=back_recv_sem.at[shift],
            device_id=there,
            device_id_type=MESH,
        ).start()
        return carry

    def spread(block):
        for step in range(1, groups):
            pltpu.make_async_remote_copy(
                src_ref=back_recv.at[0, block_rows(block)],
                dst_ref=back_recv.at[step, block_rows(block)],
                send_sem=spread_send_sem.at[step],
                recv_sem=spread_recv_sem.at[step],
                device_id=target(step, 0),
                device_id_type=MESH,
            ).start()

    def pass_on(shift, carry):
        block = lax.rem(my_block - shift + blocks, blocks)
        arrived = back_recv.at[0, block_rows(block)]
        wait_bytes(arrived, back_recv_sem.at[shift])
        spread(block)
        return carry

    lax.fori_loop(1, blocks, return_to, 0)
    back_recv[0, block_rows(my_block)] = back_send[my_block]
    spread(my_block)
    lax.fori_loop(1, blocks, pass_on, 0)
    applied[...] = jnp.zeros_like(applied)

    def combine(step):
        group = lax.rem(my_band - step + groups, groups)
        harm = contract(back_recv[step], colat[...], 0, 0)
        held = [slot_row(group * slots + slot) for slot in range(slots)]
        for stokes in range(STOKES):
            sums = [applied[comp * STOKES + stokes] for comp in range(COMP)]
            for slot in range(slots):
                mix, beam = held[slot]
                first = (slot * STOKES + stokes) * rows
                term = harm[first : first + rows, :] * beam
                sums = [sums[comp] + mix[comp] * term for comp in range(COMP)]
            for comp in range(COMP):
                applied[comp * STOKES + stokes] = sums[comp]

    combine(0)

    def combine_step(step, carry):
        wait_bytes(back_recv.at[step], spread_recv_sem.at[step])
        combine(step)
        return carry

    lax.fori_loop(1, groups, combine_step, 0)

    curvature = jnp.zeros((rows, l_local), jnp.float32)
    crossed = jnp.zeros((rows, l_local), jnp.float32)
    squared = jnp.zeros((rows, l_local), jnp.float32)
    for field in range(FIELDS):
        held = direction[field]
        value = inv_spec[field : field + 1] * held + applied[field] * tri[...]
        applied[field] = value
        scaled = precond[field : field + 1] * value
        curvature = curvature + held * value
        crossed = crossed + residual[field] * scaled
        squared = squared + value * scaled

    def lane_sums(value):
        row = jnp.sum(value, axis=0, keepdims=True)
        return functools.reduce(
            jnp.add, [row[:, at : at + 128] for at in range(0, l_local, 128)]
        )

    stats[0] = jnp.concatenate(
        [lane_sums(v) for v in (residual_sum, curvature, crossed, squared)]
        + [jnp.zeros((4, 128), jnp.float32)],
        axis=0,
    )

    def tell(flat, carry):
        pltpu.make_async_remote_copy(
            src_ref=stats.at[0],
            dst_ref=stats.at[flat],
            send_sem=stat_send_sem,
            recv_sem=stat_recv_sem,
            device_id=target(flat // blocks, flat % blocks),
            device_id_type=MESH,
        ).start()
        return carry

    lax.fori_loop(1, groups * blocks, tell, 0)
    wait_bytes(stats.at[1 : groups * blocks], stat_recv_sem)
    summed = jnp.sum(jnp.sum(stats[...], axis=0), axis=1, keepdims=True)
    wide = [jnp.broadcast_to(summed[at : at + 1], (1, l_local)) for at in range(4)]
    step_size = wide[0] / wide[1]
    norm_new = wide[0] - 2.0 * step_size * wide[2] + step_size * step_size * wide[3]
    step_row[...] = step_size
    ratio_row[...] = norm_new / wide[0]

    wait_bytes(stats.at[1 : groups * blocks], stat_send_sem)
    wait_bytes(joint.at[0:rest], turn_send_sem)
    wait_bytes(joint.at[0:rest], back_send_sem)
    for step in range(1, groups):
        wait_bytes(send.at[step], send_sem.at[step])
        wait_bytes(back_recv.at[step], spread_send_sem.at[step])


def on_device(
    solution,
    residual,
    direction,
    precond,
    inv_spec,
    mixing,
    beams,
    slot_band,
    m_order,
    cycle_order,
    inv_noise,
    pix_mask,
):
    groups = lax.axis_size("band")
    blocks = lax.axis_size("blk")
    m_local, l_local = direction.shape[2:]
    rows = 2 * m_local
    modes = m_order.shape[0]
    cycle_total = cycle_order.shape[0]
    slots, _, r_local, phi_total = inv_noise.shape
    pairs = slots * STOKES
    devices = groups * blocks

    vmem = pl.BlockSpec(memory_space=pltpu.VMEM)
    smem = pl.BlockSpec(memory_space=pltpu.SMEM)
    bf16, f32 = jnp.bfloat16, jnp.float32
    field_shape = (FIELDS, rows, l_local)
    dma = pltpu.SemaphoreType.DMA
    sizes = (groups, blocks, slots, l_local * groups, modes, phi_total)
    applied, step_row, ratio_row = pl.pallas_call(
        functools.partial(kernel, sizes),
        out_shape=(
            jax.ShapeDtypeStruct(field_shape, f32),
            jax.ShapeDtypeStruct((1, l_local), f32),
            jax.ShapeDtypeStruct((1, l_local), f32),
        ),
        in_specs=[vmem] * 4 + [smem] * 4 + [vmem] * 3,
        out_specs=(vmem, vmem, vmem),
        scratch_shapes=[
            pltpu.VMEM((rows, l_local), f32),
            pltpu.VMEM(field_shape, f32),
            pltpu.VMEM((cycle_total, l_local), bf16),
            pltpu.VMEM((pairs * rows, l_local), bf16),
            pltpu.VMEM((groups, cycle_total, pairs * rows), bf16),
            pltpu.VMEM((groups, cycle_total, pairs * rows), bf16),
            pltpu.VMEM((cycle_total, pairs * rows), bf16),
            pltpu.VMEM((cycle_total, pairs * rows), bf16),
            pltpu.VMEM((blocks * rows, LANES), bf16),
            pltpu.VMEM((pairs * r_local, blocks * rows), bf16),
            pltpu.VMEM((pairs * r_local, blocks * rows), f32),
            pltpu.VMEM((blocks, r_local, pairs * rows), bf16),
            pltpu.VMEM((groups, cycle_total, pairs * rows), bf16),
            pltpu.VMEM((devices, 8, 128), f32),
            dma((groups,)),
            dma((groups,)),
            dma,
            dma,
            dma,
            dma((blocks,)),
            dma((groups,)),
            dma((groups,)),
            dma,
            dma,
        ],
        compiler_params=pltpu.CompilerParams(
            collective_id=0, has_side_effects=True, vmem_limit_bytes=60 * 1024 * 1024
        ),
    )(
        direction.reshape(field_shape),
        residual.reshape(field_shape),
        precond,
        inv_spec,
        mixing.T,
        slot_band,
        m_order,
        cycle_order,
        beams,
        inv_noise.reshape(pairs, r_local, phi_total),
        pix_mask,
    )
    applied = applied.reshape(direction.shape)
    step_size, ratio = (row[:, None, None, :] for row in (step_row, ratio_row))
    precond_full = precond[:, None, None, :]
    solution_next = solution + step_size * direction
    residual_next = residual - step_size * applied
    direction_next = precond_full * residual_next + ratio * direction
    return (solution_next, residual_next, direction_next)


def solution(mesh):
    field = P(None, None, "blk", "band")
    return jax.shard_map(
        on_device,
        mesh=mesh,
        in_specs=(
            field,
            field,
            field,
            P(None, "band"),
            P(None, "band"),
            P(),
            P(),
            P(),
            P(),
            P(),
            P("band", None, "blk", None),
            P("blk", None),
        ),
        out_specs=(field, field, field),
        check_vma=False,
    )
```

```python
import functools
import math

import jax
import jax.numpy as jnp
from jax import lax
from jax.experimental import pallas as pl
from jax.experimental.pallas import tpu as pltpu
from jax.sharding import PartitionSpec as P

COMP = 3
STOKES = 3
FIELDS = 9
BANDS = 9
LANES = 512
MESH = pl.DeviceIdType.MESH


def wave(phase, quarter):
    folded = jnp.abs(phase - 2 * quarter) - quarter
    x = folded.astype(jnp.float32) * (math.pi / (2 * quarter))
    x2 = x * x
    series = -1.0 / 39916800.0
    for coefficient in (1.0 / 362880.0, -1.0 / 5040.0, 1.0 / 120.0, -1.0 / 6.0, 1.0):
        series = series * x2 + coefficient
    return x * series


def wrapped(value, period):
    if period & (period - 1) == 0:
        return value & (period - 1)
    return lax.rem(value, period)


def contract(left, right, left_dim, right_dim):
    return lax.dot_general(
        left, right, (((left_dim,), (right_dim,)), ((), ())), preferred_element_type=jnp.float32
    )


def wait_bytes(ref, sem):
    pltpu.make_async_copy(ref, ref, sem).wait()


def kernel(
    sizes,
    direction,
    residual_in,
    precond,
    inv_spec,
    mixing,
    slot_band,
    m_order,
    cycle_order,
    beams,
    noise,
    mask,
    applied_out,
    step_row,
    ratio_row,
    residual,
    applied,
    tri,
    halved,
    colat,
    amps,
    send,
    recv,
    joint,
    turned,
    azim,
    side,
    back,
    back_send,
    back_recv,
    stats,
    send_sem,
    recv_sem,
    turn_send_sem,
    turn_recv_sem,
    back_send_sem,
    back_recv_sem,
    spread_send_sem,
    spread_recv_sem,
    stat_send_sem,
    stat_recv_sem,
    local_sem,
):
    groups, blocks, slots, l_total, modes, phi_total = sizes
    rows, l_local = direction.shape[1:]
    cycle_total = cycle_order.shape[0]
    r_local = cycle_total // blocks
    pairs = slots * STOKES
    per_lane = 128 // rows
    my_band = lax.axis_index("band")
    my_block = lax.axis_index("blk")

    high, low, half = my_band // 2, my_band % 2, groups // 2

    def target(step, shift):
        band = (high + step // 2) % half * 2 + (low + step) % 2
        return (band, lax.rem(my_block + shift, blocks))

    def origin(step):
        return (high - step // 2 + half) % half * 2 + (low + step) % 2

    load = pltpu.make_async_copy(residual_in, residual, local_sem.at[0])
    load.start()

    barrier = pltpu.get_barrier_semaphore()

    def greet(flat, carry):
        pl.semaphore_signal(
            barrier, inc=1, device_id=target(flat // blocks, flat % blocks), device_id_type=MESH
        )
        return carry

    lax.fori_loop(1, groups * blocks, greet, 0)

    def slot_row(at):
        band = slot_band[at]
        filled = jnp.where(band < BANDS, 1.0, 0.0)
        held = jnp.minimum(band, BANDS - 1)
        columns = pl.ds(pl.multiple_of(my_band * l_local, l_local), l_local)
        mix = [filled * mixing[comp, held] for comp in range(COMP)]
        return (mix, beams[pl.ds(held, 1), columns])

    def column(ref, first, count, width):
        place = lax.broadcasted_iota(jnp.int32, (8, 128), 0)
        pieces = []
        for at in range(0, count, 8):
            piece = jnp.full((8, 128), ref[first + at], jnp.int32)
            for inner in range(1, 8):
                piece = jnp.where(place == inner, ref[first + at + inner], piece)
            pieces.append(piece)
        tall = jnp.concatenate(pieces, axis=0)
        return jnp.concatenate([tall] * (width // 128), axis=1)

    l_index = my_band * l_local + lax.broadcasted_iota(jnp.int32, (1, l_local), 1)
    my_orders = column(m_order, my_block * (rows // 2), rows // 2, l_local)
    tri[...] = jnp.where(l_index >= jnp.concatenate([my_orders, my_orders], axis=0), 1.0, 0.0)
    for field in range(FIELDS):
        halved[field] = direction[field].astype(jnp.bfloat16).astype(jnp.float32) * tri[...]

    def colat_rows(at, carry):
        at_rows = pl.ds(pl.multiple_of(at * 64, 64), 64)
        phase = wrapped(l_index * (2 * column(cycle_order, at * 64, 64, l_local) + 1), 4 * cycle_total)
        colat[at_rows, :] = (wave(phase, cycle_total) / math.sqrt(l_total)).astype(jnp.bfloat16)
        return carry

    lax.fori_loop(0, cycle_total // 64, colat_rows, 0)

    def transform(step):
        group = target(step, 0)[0]
        for slot in range(slots):
            at = group * slots + slot
            mix, beam = slot_row(at)
            for stokes in range(STOKES):
                mixed = mix[0] * halved[stokes]
                for comp in range(1, COMP):
                    mixed = mixed + mix[comp] * halved[comp * STOKES + stokes]
                first = (slot * STOKES + stokes) * rows
                amps[first : first + rows, :] = (mixed * beam).astype(jnp.bfloat16)
        send[step] = contract(colat[...], amps[...], 1, 1).astype(jnp.bfloat16)

    def block_rows(block):
        return pl.ds(pl.multiple_of(block * r_local, r_local), r_local)

    def ship(step):
        pltpu.make_async_remote_copy(
            src_ref=send.at[step],
            dst_ref=recv.at[step],
            send_sem=send_sem.at[step],
            recv_sem=recv_sem.at[step],
            device_id=target(step, 0),
            device_id_type=MESH,
        ).start()

    transform(groups - 1)
    pl.semaphore_wait(barrier, groups * blocks - 1)
    ship(groups - 1)

    def group_step(at, carry):
        step = groups - at
        transform(step)
        ship(step)
        return carry

    lax.fori_loop(2, groups, group_step, 0)
    transform(0)

    def fill_azim(chunk):
        cell = chunk * LANES + lax.broadcasted_iota(jnp.int32, (1, LANES), 1)

        def one(at, carry):
            at_rows = pl.ds(pl.multiple_of(at * 2 * rows, 2 * rows), 2 * rows)
            phases = []
            for inner in range(2):
                orders = column(m_order, (at * 2 + inner) * (rows // 2), rows // 2, LANES)
                phases += [orders * cell, orders * cell + phi_total // 4]
            phase = wrapped(jnp.concatenate(phases, axis=0), phi_total)
            azim[at_rows, :] = (wave(phase, phi_total // 4) / math.sqrt(modes)).astype(jnp.bfloat16)
            return carry

        lax.fori_loop(0, blocks // 2, one, 0)

    chunks = phi_total // LANES
    if chunks == 1:
        fill_azim(0)
    rest = (blocks - 1) * r_local
    for step in range(1, groups):
        wait_bytes(recv.at[step], recv_sem.at[step])

    def add_up(at, carry):
        at_rows = block_rows(at)
        total = send[0, at_rows, :].astype(jnp.float32)
        for step in range(1, groups):
            total = total + recv[step, at_rows, :].astype(jnp.float32)
        joint[at_rows, :] = total.astype(jnp.bfloat16)
        return carry

    lax.fori_loop(0, blocks, add_up, 0)

    def turn(shift, carry):
        there = target(0, shift)
        pltpu.make_async_remote_copy(
            src_ref=joint.at[block_rows(there[1])],
            dst_ref=turned.at[block_rows(shift)],
            send_sem=turn_send_sem,
            recv_sem=turn_recv_sem,
            device_id=there,
            device_id_type=MESH,
        ).start()
        return carry

    lax.fori_loop(1, blocks, turn, 0)
    turned[0:r_local] = joint[block_rows(my_block)]
    load.wait()
    residual_sum = jnp.zeros((rows, l_local), jnp.float32)
    for field in range(FIELDS):
        residual_sum = residual_sum + residual[field] * (
            precond[field : field + 1] * residual[field]
        )
    wait_bytes(turned.at[r_local:cycle_total], turn_recv_sem)

    def gather(at, carry):
        parts = []
        for inner in range(per_lane):
            block = at * per_lane + inner
            rows_at = block_rows(lax.rem(my_block - block + blocks, blocks))
            parts.append(turned[rows_at, :].astype(jnp.float32))
        columns = pl.ds(pl.multiple_of(at * 128, 128), 128)
        for pair in range(pairs):
            picked = [part[:, pair * rows : (pair + 1) * rows] for part in parts]
            joined = jnp.concatenate(picked, axis=1).astype(jnp.bfloat16)
            side[pair * r_local : (pair + 1) * r_local, columns] = joined
        return carry

    lax.fori_loop(0, blocks // per_lane, gather, 0)

    def weigh(chunk):
        columns = pl.ds(pl.multiple_of(chunk * LANES, LANES), LANES)
        sky = contract(side[...], azim[...], 1, 0).reshape(pairs, r_local, LANES)
        weight = noise[:, :, columns] * mask[:, columns].astype(jnp.float32)[None]
        weighted = (weight * sky).astype(jnp.bfloat16).reshape(pairs * r_local, LANES)
        return contract(weighted, azim[...], 1, 1)

    if chunks == 1:
        back[...] = weigh(0)
    else:
        back[...] = jnp.zeros_like(back)

        def one_chunk(chunk, carry):
            fill_azim(chunk)
            back[...] += weigh(chunk)
            return carry

        lax.fori_loop(0, chunks, one_chunk, 0)

    def scatter(at, carry):
        columns = pl.ds(pl.multiple_of(at * 128, 128), 128)
        wide = [back[pair * r_local : (pair + 1) * r_local, columns] for pair in range(pairs)]
        for inner in range(per_lane):
            picked = [part[:, inner * rows : (inner + 1) * rows] for part in wide]
            joined = jnp.concatenate(picked, axis=1).astype(jnp.bfloat16)
            back_send[at * per_lane + inner] = joined
        return carry

    lax.fori_loop(0, blocks // per_lane, scatter, 0)

    def return_to(shift, carry):
        there = target(0, shift)
        pltpu.make_async_remote_copy(
            src_ref=back_send.at[there[1]],
            dst_ref=back_recv.at[0, block_rows(my_block)],
            send_sem=back_send_sem,
            recv_sem=back_recv_sem.at[shift],
            device_id=there,
            device_id_type=MESH,
        ).start()
        return carry

    def spread(block, steps):
        for step in steps:
            pltpu.make_async_remote_copy(
                src_ref=back_recv.at[0, block_rows(block)],
                dst_ref=back_recv.at[step, block_rows(block)],
                send_sem=spread_send_sem.at[step],
                recv_sem=spread_recv_sem.at[step],
                device_id=target(step, 0),
                device_id_type=MESH,
            ).start()

    def pass_on(shift, carry):
        block = lax.rem(my_block - shift + blocks, blocks)
        arrived = back_recv.at[0, block_rows(block)]
        wait_bytes(arrived, back_recv_sem.at[shift])
        spread(block, near)
        return carry

    def pass_far(block, carry):
        spread(block, far)
        return carry

    near, far = range(1, groups - 1), range(groups - 1, groups)

    lax.fori_loop(1, blocks, return_to, 0)
    back_recv[0, block_rows(my_block)] = back_send[my_block]
    spread(my_block, near)
    lax.fori_loop(1, blocks, pass_on, 0)
    lax.fori_loop(0, blocks, pass_far, 0)
    applied[...] = jnp.zeros_like(applied)

    def combine(step):
        group = origin(step)
        harm = contract(back_recv[step], colat[...], 0, 0)
        held = [slot_row(group * slots + slot) for slot in range(slots)]
        for stokes in range(STOKES):
            sums = [applied[comp * STOKES + stokes] for comp in range(COMP)]
            for slot in range(slots):
                mix, beam = held[slot]
                first = (slot * STOKES + stokes) * rows
                term = harm[first : first + rows, :] * beam
                sums = [sums[comp] + mix[comp] * term for comp in range(COMP)]
            for comp in range(COMP):
                applied[comp * STOKES + stokes] = sums[comp]

    combine(0)

    def combine_step(step, carry):
        wait_bytes(back_recv.at[step], spread_recv_sem.at[step])
        combine(step)
        return carry

    lax.fori_loop(1, groups, combine_step, 0)

    curvature = jnp.zeros((rows, l_local), jnp.float32)
    crossed = jnp.zeros((rows, l_local), jnp.float32)
    squared = jnp.zeros((rows, l_local), jnp.float32)
    for field in range(FIELDS):
        held = direction[field]
        value = inv_spec[field : field + 1] * held + applied[field] * tri[...]
        applied[field] = value
        scaled = precond[field : field + 1] * value
        curvature = curvature + held * value
        crossed = crossed + residual[field] * scaled
        squared = squared + value * scaled

    def lane_sums(value):
        row = jnp.sum(value, axis=0, keepdims=True)
        return functools.reduce(
            jnp.add, [row[:, at : at + 128] for at in range(0, l_local, 128)]
        )

    stats[0] = jnp.concatenate(
        [lane_sums(v) for v in (residual_sum, curvature, crossed, squared)]
        + [jnp.zeros((4, 128), jnp.float32)],
        axis=0,
    )

    def tell(flat, carry):
        pltpu.make_async_remote_copy(
            src_ref=stats.at[0],
            dst_ref=stats.at[flat],
            send_sem=stat_send_sem,
            recv_sem=stat_recv_sem,
            device_id=target(flat // blocks, flat % blocks),
            device_id_type=MESH,
        ).start()
        return carry

    lax.fori_loop(1, groups * blocks, tell, 0)
    store = pltpu.make_async_copy(applied, applied_out, local_sem.at[1])
    store.start()
    wait_bytes(stats.at[1 : groups * blocks], stat_recv_sem)
    summed = jnp.sum(jnp.sum(stats[...], axis=0), axis=1, keepdims=True)
    wide = [jnp.broadcast_to(summed[at : at + 1], (1, l_local)) for at in range(4)]
    step_size = wide[0] / wide[1]
    norm_new = wide[0] - 2.0 * step_size * wide[2] + step_size * step_size * wide[3]
    step_row[...] = step_size
    ratio_row[...] = norm_new / wide[0]

    store.wait()
    wait_bytes(stats.at[1 : groups * blocks], stat_send_sem)
    wait_bytes(joint.at[0:rest], turn_send_sem)
    wait_bytes(joint.at[0:rest], back_send_sem)
    for step in range(1, groups):
        wait_bytes(send.at[step], send_sem.at[step])
        wait_bytes(back_recv.at[step], spread_send_sem.at[step])


def on_device(
    solution,
    residual,
    direction,
    precond,
    inv_spec,
    mixing,
    beams,
    slot_band,
    m_order,
    cycle_order,
    inv_noise,
    pix_mask,
):
    groups = lax.axis_size("band")
    blocks = lax.axis_size("blk")
    m_local, l_local = direction.shape[2:]
    rows = 2 * m_local
    modes = m_order.shape[0]
    cycle_total = cycle_order.shape[0]
    slots, _, r_local, phi_total = inv_noise.shape
    pairs = slots * STOKES
    devices = groups * blocks

    vmem = pl.BlockSpec(memory_space=pltpu.VMEM)
    whole = pl.BlockSpec(memory_space=pl.ANY)
    smem = pl.BlockSpec(memory_space=pltpu.SMEM)
    bf16, f32 = jnp.bfloat16, jnp.float32
    field_shape = (FIELDS, rows, l_local)
    dma = pltpu.SemaphoreType.DMA
    sizes = (groups, blocks, slots, l_local * groups, modes, phi_total)
    applied, step_row, ratio_row = pl.pallas_call(
        functools.partial(kernel, sizes),
        out_shape=(
            jax.ShapeDtypeStruct(field_shape, f32),
            jax.ShapeDtypeStruct((1, l_local), f32),
            jax.ShapeDtypeStruct((1, l_local), f32),
        ),
        in_specs=[vmem, whole, vmem, vmem] + [smem] * 4 + [vmem] * 3,
        out_specs=(whole, vmem, vmem),
        scratch_shapes=[
            pltpu.VMEM(field_shape, f32),
            pltpu.VMEM(field_shape, f32),
            pltpu.VMEM((rows, l_local), f32),
            pltpu.VMEM(field_shape, f32),
            pltpu.VMEM((cycle_total, l_local), bf16),
            pltpu.VMEM((pairs * rows, l_local), bf16),
            pltpu.VMEM((groups, cycle_total, pairs * rows), bf16),
            pltpu.VMEM((groups, cycle_total, pairs * rows), bf16),
            pltpu.VMEM((cycle_total, pairs * rows), bf16),
            pltpu.VMEM((cycle_total, pairs * rows), bf16),
            pltpu.VMEM((blocks * rows, LANES), bf16),
            pltpu.VMEM((pairs * r_local, blocks * rows), bf16),
            pltpu.VMEM((pairs * r_local, blocks * rows), f32),
            pltpu.VMEM((blocks, r_local, pairs * rows), bf16),
            pltpu.VMEM((groups, cycle_total, pairs * rows), bf16),
            pltpu.VMEM((devices, 8, 128), f32),
            dma((groups,)),
            dma((groups,)),
            dma,
            dma,
            dma,
            dma((blocks,)),
            dma((groups,)),
            dma((groups,)),
            dma,
            dma,
            dma((2,)),
        ],
        compiler_params=pltpu.CompilerParams(
            collective_id=0, has_side_effects=True, vmem_limit_bytes=60 * 1024 * 1024
        ),
    )(
        direction.reshape(field_shape),
        residual.reshape(field_shape),
        precond,
        inv_spec,
        mixing.T,
        slot_band,
        m_order,
        cycle_order,
        beams,
        inv_noise.reshape(pairs, r_local, phi_total),
        pix_mask,
    )
    applied = applied.reshape(direction.shape)
    step_size, ratio = (row[:, None, None, :] for row in (step_row, ratio_row))
    precond_full = precond[:, None, None, :]
    solution_next = solution + step_size * direction
    residual_next = residual - step_size * applied
    direction_next = precond_full * residual_next + ratio * direction
    return (solution_next, residual_next, direction_next)


def solution(mesh):
    field = P(None, None, "blk", "band")
    return jax.shard_map(
        on_device,
        mesh=mesh,
        in_specs=(
            field,
            field,
            field,
            P(None, "band"),
            P(None, "band"),
            P(),
            P(),
            P(),
            P(),
            P(),
            P("band", None, "blk", None),
            P("blk", None),
        ),
        out_specs=(field, field, field),
        check_vma=False,
    )
```
